32 devices in a mesh: row: 8 (over y, x, core), col: 4 (over z).
Axes of the slice: x: 2, y: 2, z: 4, core: 2. Of those that a mesh axis runs over, the one named last changes fastest.
Arguments:
- vectors_window: float32 [32, 8, 64, 1024], P(None, 'row', None, 'col'), may hold values from -6 to 6
- column_strip: float32 [32, 8, 64, 1024], P(None, 'row', None, 'col'), may hold values from -6 to 6
- row_strip: float32 [1024, 32, 4, 128], P('row', None, 'col'), may hold values from -6 to 6
- factor: float32 [1024, 1024], P('row', 'col'), may hold values from -2 to 2
- window_start: int32 [1], replicated, may hold values from 1 to 15360
- deflated: int32 [1], replicated, may hold values from 0 to 512
Outputs:
- vectors_updated: float32 [32, 8, 64, 1024], P(None, 'row', None, 'col')
- column_updated: float32 [32, 8, 64, 1024], P(None, 'row', None, 'col')
- row_updated: float32 [1024, 32, 4, 128], P('row', None, 'col')
The draws below stay inside these ranges and needn't reach their ends.
All inputs are finite; a program needn't handle non-finite values.
Results may differ from the reference program's by a relative error of at most 0.0003.
Values sent between devices are 32-bit elements; how exact they have to be, the bound alone decides.
A program may use at most 64 MiB of HBM per device.

```python
import math
import jax
import jax.numpy as jnp
from jax import lax

W = 1024
BLK = 64
CBLK = 128
ROUNDS = 32
N = 16384
CROUNDS = 32
N_ROW = 8
N_COL = 4


def draw_factor(key, part):
    noise_key, scale_key = jax.random.split(key)
    positions = jnp.arange(W, dtype=jnp.float32) / (W - 1)
    spread = jnp.exp(jax.random.uniform(scale_key, (W,), jnp.float32, -1.15, 1.15))
    entries = jnp.clip(jax.random.normal(noise_key, (W, W), jnp.float32), -5.0, 5.0)
    column_scale = spread * jnp.exp(0.5 * math.log(3.0) * positions) / 1.5
    return (entries * column_scale[None, :] / math.sqrt(W)).astype(jnp.float32)


def block_levels(rng, dims, cuts, smallest, top_value):
    def one(dim, parts):
        steps = jax.random.uniform(jax.random.fold_in(jax.random.fold_in(rng, 6), dim), (parts,), jnp.float32, smallest / len(cuts), top_value / len(cuts))
        return jnp.repeat(jnp.exp(steps), dims[dim] // parts).reshape((-1,) + (1,) * (len(dims) - dim - 1))

    gain = one(*cuts[0])
    for cut in cuts[1:]:
        gain = gain * one(*cut)
    return gain


def normal_values(rng, shape, scale, most, shards=(), kind=jnp.bfloat16):
    gain = block_levels(rng, shape, shards, -0.22, 0.18) if shards else 1.0
    result = jax.random.normal(rng, shape, jnp.float32) * scale * gain
    return jnp.minimum(jnp.maximum(result, -most), most).astype(kind)


def setup_inputs(seed: int = 0) -> dict:
    streams_of = jax.random.split(jax.random.key(seed), 7)
    vectors_window = normal_values(streams_of[0], (ROUNDS, N_ROW, BLK, W), 1.0, 6.0, ((1, 8), (3, 4)), jnp.float32)
    column_strip = normal_values(streams_of[1], (ROUNDS, N_ROW, BLK, W), 1.0, 6.0, ((1, 8), (3, 4)), jnp.float32)
    row_strip = normal_values(streams_of[2], (W, CROUNDS, N_COL, CBLK), 1.0, 6.0, ((0, 8), (2, 4)), jnp.float32)
    factor = draw_factor(jax.random.fold_in(streams_of[6], 71), 0)
    window_start = jax.random.randint(streams_of[4], (1,), 1, N - W + 1).astype(jnp.int32)
    deflated = jax.random.randint(streams_of[5], (1,), 0, W // 2 + 1).astype(jnp.int32)
    return dict(vectors_window=vectors_window, column_strip=column_strip, row_strip=row_strip, factor=factor, window_start=window_start, deflated=deflated)


def reflect(factor, deflated):
    columns = jnp.arange(W, dtype=jnp.int32)
    kept_count = W - deflated[0]
    spike_row = jnp.where(columns < kept_count, factor[0], 0.0)
    squares = jnp.sum(spike_row * spike_row)
    corner = factor[0, 0]
    magnitude = jnp.sqrt(squares + 1e-06)
    signum = jnp.where(corner >= 0, 1.0, -1.0)
    vector = spike_row + jnp.where(columns == 0, signum * magnitude, 0.0)
    denominator = squares + 2.0 * jnp.abs(corner) * magnitude + magnitude * magnitude
    scaling = 2.0 / denominator
    reflected_image = jnp.dot(factor, vector, precision=lax.Precision.HIGHEST)
    return factor - scaling * reflected_image[:, None] * vector[None, :]

def reference(vectors_window, column_strip, row_strip, factor, window_start, deflated):
    highest = lax.Precision.HIGHEST
    rotation = reflect(factor, deflated)
    start_row = window_start[0]
    z_matrix = vectors_window.reshape(N, W)
    vectors_updated = jnp.dot(z_matrix, rotation, precision=highest).reshape(vectors_window.shape)
    strip_matrix = column_strip.reshape(N, W)
    turned = jnp.dot(strip_matrix, rotation, precision=highest)
    row_number = jnp.arange(N, dtype=jnp.int32)
    column_updated = jnp.where(row_number[:, None] < start_row, turned, strip_matrix).reshape(column_strip.shape)
    row_panel = row_strip.reshape(W, N)
    rotated_rows = lax.dot_general(rotation, row_panel, (((0,), (0,)), ((), ())), precision=highest)
    column_number = jnp.arange(N, dtype=jnp.int32)
    row_updated = jnp.where(column_number[None, :] >= start_row + W, rotated_rows, row_panel).reshape(row_strip.shape)
    return (vectors_updated, column_updated, row_updated)
```

```python
import functools
import jax
import jax.numpy as jnp
from jax import lax
from jax.experimental import pallas as pl
from jax.experimental.pallas import tpu as pltpu
from jax.sharding import PartitionSpec as P

MESH = pl.DeviceIdType.MESH


def drain(ref, sem):
    pltpu.make_async_copy(ref, ref, sem).wait()


def split(x):
    high = x.astype(jnp.bfloat16)
    low = (x - high.astype(jnp.float32)).astype(jnp.bfloat16)
    return high, low


def kernel(
    nr, nc, s_groups, r_first,
    deflated, z, s, r, f,
    zo, so, ro,
    fbuf, rot, rh, rl, th, tl,
    zb, sb, rb, zq, sq, rq,
    f_col_send, f_col_recv, f_row_send, f_row_recv, f_pass_send, f_pass_recv,
    in_send, out_send, out_recv, z_recv, s_recv, r_recv,
):
    row = lax.axis_index("row")
    col = lax.axis_index("col")
    z_groups = z.shape[0] // nc
    r_groups = r.shape[0] // nr
    width = nc * f.shape[1]
    tall = f.shape[0]
    wide = f.shape[1]
    chips = nr // 2
    sibling = row + 1 - 2 * lax.rem(row, 2)

    def col_peer(d):
        return lax.rem(col + d, nc)

    def row_peer(d):
        return lax.rem(row + d, nr)

    def send(src, dst, send_sem, recv_sem, target):
        copy = pltpu.make_async_remote_copy(
            src_ref=src, dst_ref=dst, send_sem=send_sem, recv_sem=recv_sem,
            device_id=target, device_id_type=MESH,
        )
        copy.start()
        return copy

    barrier = pltpu.get_barrier_semaphore()
    for d in range(1, nc):
        pl.semaphore_signal(barrier, inc=1, device_id={"col": col_peer(d)}, device_id_type=MESH)
    for d in range(1, nr):
        pl.semaphore_signal(barrier, inc=1, device_id={"row": row_peer(d)}, device_id_type=MESH)
    pl.semaphore_wait(barrier, nc + nr - 2)

    order = list(range(1, nc))
    for d in order:
        send(f, fbuf.at[row, col], f_col_send, f_col_recv, {"col": col_peer(d)})

    @pl.loop(0, z_groups)
    def _(g):
        for d in order:
            p = col_peer(d)
            send(z.at[g * nc + p], zb.at[g, col], in_send.at[0], z_recv.at[g], {"col": p})

    fbuf[row, col] = f[...]
    drain(fbuf.at[0, pl.ds(0, nc - 1)], f_col_recv)
    send(fbuf.at[row], fbuf.at[row], f_row_send, f_pass_recv.at[0], {"row": sibling})
    for d in range(1, chips):
        send(fbuf.at[row], fbuf.at[row], f_row_send, f_row_recv.at[d], {"row": row_peer(2 * d)})

    if r_first < r_groups:
        @pl.loop(r_first, r_groups)
        def _(g):
            for d in range(1, nr):
                p = row_peer(d)
                send(r.at[g * nr + p], rb.at[g, row], in_send.at[2], r_recv.at[g], {"row": p})

    if s_groups:
        @pl.loop(0, s_groups)
        def _(g):
            for d in order:
                p = col_peer(d)
                send(s.at[g * nc + p], sb.at[g, col], in_send.at[1], s_recv.at[g], {"col": p})

    for d in range(1, chips):
        drain(fbuf.at[0], f_row_recv.at[d])
        origin = row_peer(nr - 2 * d)
        send(fbuf.at[origin], fbuf.at[origin], f_pass_send, f_pass_recv.at[d], {"row": sibling})
    for d in range(chips):
        drain(fbuf.at[0], f_pass_recv.at[d])

    kept = width - deflated[0]
    squares = jnp.zeros((1, 1), jnp.float32)
    spikes = []
    for c in range(nc):
        lane = lax.broadcasted_iota(jnp.int32, (1, wide), 1) + c * wide
        part = jnp.where(lane < kept, fbuf[0, c, 0:1, :], 0.0)
        squares = squares + jnp.sum(part * part, axis=1, keepdims=True)
        spikes.append((lane, part))
    corner = fbuf[0, 0, 0:1, 0:1]
    magnitude = jnp.sqrt(squares + 1e-06)
    shift = jnp.where(corner >= 0, 1.0, -1.0) * magnitude
    scaling = 2.0 / (squares + 2.0 * jnp.abs(corner) * magnitude + magnitude * magnitude)
    vector = [part + jnp.where(lane == 0, shift, 0.0) for lane, part in spikes]

    @pl.loop(0, nr)
    def _(i):
        image = jnp.zeros((tall, 1), jnp.float32)
        for c in range(nc):
            image = image + jnp.sum(fbuf[i, c] * vector[c], axis=1, keepdims=True)
        image = image * scaling
        rows = pl.ds(pl.multiple_of(i * tall, tall), tall)
        for c in range(nc):
            rot[rows, c * wide:(c + 1) * wide] = fbuf[i, c] - image * vector[c]

    @pl.loop(0, width // 128)
    def _(i):
        rows = pl.ds(pl.multiple_of(i * 128, 128), 128)
        block = rot[rows, :]
        high, low = split(block)
        rh[rows, :] = high
        rl[rows, :] = low
        if r_first < r_groups:
            high, low = split(block.T)
            th[:, rows] = high
            tl[:, rows] = low

    def panel(x, xb, xq, xo, recv, groups, k):
        blk = x.shape[1]

        def back(g):
            for d in order:
                p = col_peer(d)
                send(xq.at[g, p], xo.at[g * nc + col], out_send.at[k], out_recv.at[k], {"col": p})

        @pl.loop(0, groups)
        def _(g):
            xb[g, col] = x[g * nc + col]
            drain(xb.at[g, pl.ds(0, nc - 1)], recv.at[g])
            total = jnp.zeros((blk, width), jnp.float32)
            for c in range(nc):
                high, low = split(xb[g, c])
                rows = slice(c * wide, (c + 1) * wide)
                both = jnp.dot(
                    jnp.concatenate([high, low], axis=0), rh[rows, :],
                    preferred_element_type=jnp.float32,
                )
                total = total + both[:blk] + both[blk:]
                total = total + jnp.dot(high, rl[rows, :], preferred_element_type=jnp.float32)
            for c in range(nc):
                xq[g, c] = total[:, c * wide:(c + 1) * wide]
            xo[g * nc + col] = xq[g, col]
            @pl.when(g > 0)
            def _():
                back(g - 1)

        back(groups - 1)

    panel(z, zb, zq, zo, z_recv, z_groups, 0)

    if r_first < r_groups:
        def r_back(g):
            for d in range(1, nr):
                p = row_peer(d)
                send(rq.at[g, p], ro.at[g * nr + row], out_send.at[2], out_recv.at[2], {"row": p})

        @pl.loop(r_first, r_groups)
        def _(g):
            rb[g, row] = r[g * nr + row]
            drain(rb.at[g, pl.ds(0, nr - 1)], r_recv.at[g])
            lanes = r.shape[2]
            high, low = split(rb[g].reshape(width, lanes))
            pair = jnp.concatenate([high, low], axis=1)

            @pl.loop(0, nr)
            def _(q):
                rows = pl.ds(pl.multiple_of(q * tall, tall), tall)
                both = jnp.dot(th[rows, :], pair, preferred_element_type=jnp.float32)
                rest = jnp.dot(tl[rows, :], high, preferred_element_type=jnp.float32)
                rq[g, q] = both[:, :lanes] + both[:, lanes:] + rest

            ro[g * nr + row] = rq[g, row]
            @pl.when(g > r_first)
            def _():
                r_back(g - 1)

        r_back(r_groups - 1)

    if s_groups:
        panel(s, sb, sq, so, s_recv, s_groups, 1)

    part = z_groups * (nc - 1)
    drain(zo.at[pl.ds(0, part)], out_recv.at[0])
    drain(zo.at[pl.ds(0, part)], out_send.at[0])
    drain(zo.at[pl.ds(0, part)], in_send.at[0])
    if s_groups:
        part = s_groups * (nc - 1)
        drain(so.at[pl.ds(0, part)], out_recv.at[1])
        drain(so.at[pl.ds(0, part)], out_send.at[1])
        drain(so.at[pl.ds(0, part)], in_send.at[1])
    if r_first < r_groups:
        part = (r_groups - r_first) * (nr - 1)
        drain(ro.at[pl.ds(0, part)], out_recv.at[2])
        drain(ro.at[pl.ds(0, part)], out_send.at[2])
        drain(ro.at[pl.ds(0, part)], in_send.at[2])
    drain(fbuf.at[0, pl.ds(0, nc - 1)], f_col_send)
    drain(fbuf.at[pl.ds(0, chips)], f_row_send)
    drain(fbuf.at[pl.ds(0, chips - 1)], f_pass_send)


def rotate(nr, nc, s_groups, r_first, ident, z, s, r, f, deflated):
    z_groups = z.shape[0] // nc
    r_groups = r.shape[0] // nr
    width = nc * f.shape[1]
    vmem = pl.BlockSpec(memory_space=pltpu.VMEM)
    f32 = jnp.float32
    bf16 = jnp.bfloat16
    dma = pltpu.SemaphoreType.DMA
    col_block = (nc,) + z.shape[1:]
    row_block = (nr,) + r.shape[1:]
    return pl.pallas_call(
        functools.partial(kernel, nr, nc, s_groups, r_first),
        out_shape=[jax.ShapeDtypeStruct(x.shape, f32) for x in (z, s, r)],
        in_specs=[pl.BlockSpec(memory_space=pltpu.SMEM)] + [vmem] * 4,
        out_specs=[vmem] * 3,
        scratch_shapes=[
            pltpu.VMEM((nr, nc) + f.shape, f32),
            pltpu.VMEM((width, width), f32),
            pltpu.VMEM((width, width), bf16),
            pltpu.VMEM((width, width), bf16),
            pltpu.VMEM((width, width), bf16),
            pltpu.VMEM((width, width), bf16),
            pltpu.VMEM((z_groups,) + col_block, f32),
            pltpu.VMEM((z_groups,) + col_block, f32),
            pltpu.VMEM((r_groups,) + row_block, f32),
            pltpu.VMEM((z_groups,) + col_block, f32),
            pltpu.VMEM((z_groups,) + col_block, f32),
            pltpu.VMEM((r_groups,) + row_block, f32),
            dma, dma, dma, dma((nr // 2,)), dma, dma((nr // 2,)),
            dma((3,)), dma((3,)), dma((3,)),
            dma((z_groups,)), dma((z_groups,)), dma((r_groups,)),
        ],
        compiler_params=pltpu.CompilerParams(
            collective_id=ident, has_side_effects=True, vmem_limit_bytes=60 * 1024 * 1024,
        ),
    )(deflated, z, s, r, f)


def body(vectors_window, column_strip, row_strip, factor, window_start, deflated):
    nr = lax.axis_size("row")
    nc = lax.axis_size("col")
    row_position = lax.axis_index("row")
    column_position = lax.axis_index("col")
    start_row = window_start[0]
    rounds, _, blocks, wide = vectors_window.shape
    tall, column_rounds, _, lanes = row_strip.shape
    width = nc * wide
    z = vectors_window.reshape(rounds, blocks, wide)
    s = column_strip.reshape(rounds, blocks, wide)
    flat = row_strip.reshape(tall, column_rounds, lanes)
    r = jnp.transpose(flat, (1, 0, 2))
    zo, so, ro = rotate(nr, nc, rounds // nc, 0, 0, z, s, r, factor, deflated)
    round_number = jnp.arange(rounds, dtype=jnp.int32)[:, None]
    block_number = jnp.arange(blocks, dtype=jnp.int32)[None, :]
    row_number = (round_number * nr + row_position) * blocks + block_number
    column_updated = jnp.where(row_number[:, :, None] < start_row, so, s)
    round_index = jnp.arange(column_rounds, dtype=jnp.int32)[:, None]
    lane_index = jnp.arange(lanes, dtype=jnp.int32)[None, :]
    column_number = (round_index * nc + column_position) * lanes + lane_index
    row_updated = jnp.where(
        column_number[None] >= start_row + width, jnp.transpose(ro, (1, 0, 2)), flat
    )
    return (
        zo.reshape(vectors_window.shape),
        column_updated.reshape(column_strip.shape),
        row_updated.reshape(row_strip.shape),
    )


def solution(mesh):
    return jax.shard_map(
        body,
        mesh=mesh,
        in_specs=(
            P(None, "row", None, "col"),
            P(None, "row", None, "col"),
            P("row", None, "col", None),
            P("row", "col"),
            P(),
            P(),
        ),
        out_specs=(
            P(None, "row", None, "col"),
            P(None, "row", None, "col"),
            P("row", None, "col", None),
        ),
        check_vma=False,
    )
```

```python
import functools
import jax
import jax.numpy as jnp
from jax import lax
from jax.experimental import pallas as pl
from jax.experimental.pallas import tpu as pltpu
from jax.sharding import PartitionSpec as P

MESH = pl.DeviceIdType.MESH


def drain(ref, sem):
    pltpu.make_async_copy(ref, ref, sem).wait()


def split(x):
    high = x.astype(jnp.bfloat16)
    low = (x - high.astype(jnp.float32)).astype(jnp.bfloat16)
    return high, low


def kernel(
    nr, nc, s_groups, r_first,
    deflated, z, s, r, f,
    zo, so, ro,
    fbuf, rot, rh, rl, th, tl,
    zb, sb, rb, zq, sq, rq,
    f_col_send, f_col_recv, f_row_send, f_row_recv, f_pass_send, f_pass_recv,
    in_send, out_send, out_recv, z_recv, s_recv, r_recv,
):
    row = lax.axis_index("row")
    col = lax.axis_index("col")
    z_groups = z.shape[0] // nc
    r_groups = r.shape[0] // nr
    width = nc * f.shape[1]
    tall = f.shape[0]
    wide = f.shape[1]
    chips = nr // 2
    sibling = row + 1 - 2 * lax.rem(row, 2)

    def col_peer(d):
        return lax.rem(col + d, nc)

    def row_peer(d):
        return lax.rem(row + d, nr)

    def send(src, dst, send_sem, recv_sem, target):
        copy = pltpu.make_async_remote_copy(
            src_ref=src, dst_ref=dst, send_sem=send_sem, recv_sem=recv_sem,
            device_id=target, device_id_type=MESH,
        )
        copy.start()
        return copy

    barrier = pltpu.get_barrier_semaphore()
    for d in range(1, nc):
        pl.semaphore_signal(barrier, inc=1, device_id={"col": col_peer(d)}, device_id_type=MESH)
    for d in range(1, nr):
        pl.semaphore_signal(barrier, inc=1, device_id={"row": row_peer(d)}, device_id_type=MESH)
    pl.semaphore_wait(barrier, nc + nr - 2)

    order = list(range(1, nc))
    for d in order:
        send(f, fbuf.at[row, col], f_col_send, f_col_recv, {"col": col_peer(d)})

    @pl.loop(0, z_groups)
    def _(g):
        for d in order:
            p = col_peer(d)
            send(z.at[g * nc + p], zb.at[g, col], in_send.at[0], z_recv.at[g], {"col": p})

    fbuf[row, col] = f[...]
    drain(fbuf.at[0, pl.ds(0, nc - 1)], f_col_recv)
    send(fbuf.at[row], fbuf.at[row], f_row_send, f_pass_recv.at[0], {"row": sibling})
    for d in range(1, chips):
        send(fbuf.at[row], fbuf.at[row], f_row_send, f_row_recv.at[d], {"row": row_peer(2 * d)})

    if r_first < r_groups:
        @pl.loop(r_first, r_groups)
        def _(g):
            for d in range(1, nr):
                p = row_peer(d)
                send(r.at[g * nr + p], rb.at[g, row], in_send.at[2], r_recv.at[g], {"row": p})

    if s_groups:
        @pl.loop(0, s_groups)
        def _(g):
            for d in order:
                p = col_peer(d)
                send(s.at[g * nc + p], sb.at[g, col], in_send.at[1], s_recv.at[g], {"col": p})

    for d in range(1, chips):
        drain(fbuf.at[0], f_row_recv.at[d])
        origin = row_peer(nr - 2 * d)
        send(fbuf.at[origin], fbuf.at[origin], f_pass_send, f_pass_recv.at[d], {"row": sibling})
    for d in range(chips):
        drain(fbuf.at[0], f_pass_recv.at[d])

    kept = width - deflated[0]
    squares = jnp.zeros((1, 1), jnp.float32)
    spikes = []
    for c in range(nc):
        lane = lax.broadcasted_iota(jnp.int32, (1, wide), 1) + c * wide
        part = jnp.where(lane < kept, fbuf[0, c, 0:1, :], 0.0)
        squares = squares + jnp.sum(part * part, axis=1, keepdims=True)
        spikes.append((lane, part))
    corner = fbuf[0, 0, 0:1, 0:1]
    magnitude = jnp.sqrt(squares + 1e-06)
    shift = jnp.where(corner >= 0, 1.0, -1.0) * magnitude
    scaling = 2.0 / (squares + 2.0 * jnp.abs(corner) * magnitude + magnitude * magnitude)
    vector = [part + jnp.where(lane == 0, shift, 0.0) for lane, part in spikes]

    @pl.loop(0, nr)
    def _(i):
        image = jnp.zeros((tall, 1), jnp.float32)
        for c in range(nc):
            image = image + jnp.sum(fbuf[i, c] * vector[c], axis=1, keepdims=True)
        image = image * scaling
        rows = pl.ds(pl.multiple_of(i * tall, tall), tall)
        for c in range(nc):
            rot[rows, c * wide:(c + 1) * wide] = fbuf[i, c] - image * vector[c]

    @pl.loop(0, width // 128)
    def _(i):
        rows = pl.ds(pl.multiple_of(i * 128, 128), 128)
        block = rot[rows, :]
        high, low = split(block)
        rh[rows, :] = high
        rl[rows, :] = low
        if r_first < r_groups:
            high, low = split(block.T)
            th[:, rows] = high
            tl[:, rows] = low

    def panel(x, xb, xq, xo, recv, groups, k):
        blk = x.shape[1]

        def back(g):
            for d in order:
                p = col_peer(d)
                send(xq.at[g, p], xo.at[g * nc + col], out_send.at[k], out_recv.at[k], {"col": p})

        @pl.loop(0, groups)
        def _(g):
            xb[g, col] = x[g * nc + col]
            drain(xb.at[g, pl.ds(0, nc - 1)], recv.at[g])
            total = jnp.zeros((blk, width), jnp.float32)
            for c in range(nc):
                high, low = split(xb[g, c])
                rows = slice(c * wide, (c + 1) * wide)
                both = jnp.dot(
                    jnp.concatenate([high, low], axis=0), rh[rows, :],
                    preferred_element_type=jnp.float32,
                )
                total = total + both[:blk] + both[blk:]
                total = total + jnp.dot(high, rl[rows, :], preferred_element_type=jnp.float32)
            for c in range(nc):
                xq[g, c] = total[:, c * wide:(c + 1) * wide]
            xo[g * nc + col] = xq[g, col]
            @pl.when(g > 0)
            def _():
                back(g - 1)

        back(groups - 1)

    panel(z, zb, zq, zo, z_recv, z_groups, 0)

    if r_first < r_groups:
        def r_back(g):
            for d in range(1, nr):
                p = row_peer(d)
                send(rq.at[g, p], ro.at[g * nr + row], out_send.at[2], out_recv.at[2], {"row": p})

        @pl.loop(r_first, r_groups)
        def _(g):
            rb[g, row] = r[g * nr + row]
            drain(rb.at[g, pl.ds(0, nr - 1)], r_recv.at[g])
            lanes = r.shape[2]
            high, low = split(rb[g].reshape(width, lanes))
            pair = jnp.concatenate([high, low], axis=1)

            @pl.loop(0, nr)
            def _(q):
                rows = pl.ds(pl.multiple_of(q * tall, tall), tall)
                both = jnp.dot(th[rows, :], pair, preferred_element_type=jnp.float32)
                rest = jnp.dot(tl[rows, :], high, preferred_element_type=jnp.float32)
                rq[g, q] = both[:, :lanes] + both[:, lanes:] + rest

            ro[g * nr + row] = rq[g, row]
            @pl.when(g > r_first)
            def _():
                r_back(g - 1)

        r_back(r_groups - 1)

    if s_groups:
        panel(s, sb, sq, so, s_recv, s_groups, 1)

    part = z_groups * (nc - 1)
    drain(zo.at[pl.ds(0, part)], out_recv.at[0])
    drain(zo.at[pl.ds(0, part)], out_send.at[0])
    drain(zo.at[pl.ds(0, part)], in_send.at[0])
    if s_groups:
        part = s_groups * (nc - 1)
        drain(so.at[pl.ds(0, part)], out_recv.at[1])
        drain(so.at[pl.ds(0, part)], out_send.at[1])
        drain(so.at[pl.ds(0, part)], in_send.at[1])
    if r_first < r_groups:
        part = (r_groups - r_first) * (nr - 1)
        drain(ro.at[pl.ds(0, part)], out_recv.at[2])
        drain(ro.at[pl.ds(0, part)], out_send.at[2])
        drain(ro.at[pl.ds(0, part)], in_send.at[2])
    drain(fbuf.at[0, pl.ds(0, nc - 1)], f_col_send)
    drain(fbuf.at[pl.ds(0, chips)], f_row_send)
    drain(fbuf.at[pl.ds(0, chips - 1)], f_pass_send)


def rotate(nr, nc, s_groups, r_first, ident, z, s, r, f, deflated):
    z_groups = z.shape[0] // nc
    r_groups = r.shape[0] // nr
    width = nc * f.shape[1]
    vmem = pl.BlockSpec(memory_space=pltpu.VMEM)
    f32 = jnp.float32
    bf16 = jnp.bfloat16
    dma = pltpu.SemaphoreType.DMA
    col_block = (nc,) + z.shape[1:]
    row_block = (nr,) + r.shape[1:]
    return pl.pallas_call(
        functools.partial(kernel, nr, nc, s_groups, r_first),
        out_shape=[jax.ShapeDtypeStruct(x.shape, f32) for x in (z, s, r)],
        in_specs=[pl.BlockSpec(memory_space=pltpu.SMEM)] + [vmem] * 4,
        out_specs=[vmem] * 3,
        scratch_shapes=[
            pltpu.VMEM((nr, nc) + f.shape, f32),
            pltpu.VMEM((width, width), f32),
            pltpu.VMEM((width, width), bf16),
            pltpu.VMEM((width, width), bf16),
            pltpu.VMEM((width, width), bf16),
            pltpu.VMEM((width, width), bf16),
            pltpu.VMEM((z_groups,) + col_block, f32),
            pltpu.VMEM((z_groups,) + col_block, f32),
            pltpu.VMEM((r_groups,) + row_block, f32),
            pltpu.VMEM((z_groups,) + col_block, f32),
            pltpu.VMEM((z_groups,) + col_block, f32),
            pltpu.VMEM((r_groups,) + row_block, f32),
            dma, dma, dma, dma((nr // 2,)), dma, dma((nr // 2,)),
            dma((3,)), dma((3,)), dma((3,)),
            dma((z_groups,)), dma((z_groups,)), dma((r_groups,)),
        ],
        compiler_params=pltpu.CompilerParams(
            collective_id=ident, has_side_effects=True, vmem_limit_bytes=60 * 1024 * 1024,
        ),
    )(deflated, z, s, r, f)


def body(vectors_window, column_strip, row_strip, factor, window_start, deflated):
    nr = lax.axis_size("row")
    nc = lax.axis_size("col")
    row_position = lax.axis_index("row")
    column_position = lax.axis_index("col")
    start_row = window_start[0]
    rounds, _, blocks, wide = vectors_window.shape
    tall, column_rounds, _, lanes = row_strip.shape
    width = nc * wide
    z = vectors_window.reshape(rounds, blocks, wide)
    s = column_strip.reshape(rounds, blocks, wide)
    flat = row_strip.reshape(tall, column_rounds, lanes)
    r = jnp.transpose(flat, (1, 0, 2))
    group_rows = blocks * nr * nc
    group_columns = lanes * nr * nc
    groups = rounds // nc
    branches = [
        functools.partial(
            rotate, nr, nc, k, ((k - 1) * group_rows + 1 + width) // group_columns, k - 1
        )
        for k in range(1, groups + 1)
    ]
    choice = jnp.clip((start_row - 1) // group_rows, 0, groups - 1)
    zo, so, ro = lax.switch(choice, branches, z, s, r, factor, deflated)
    round_number = jnp.arange(rounds, dtype=jnp.int32)[:, None]
    block_number = jnp.arange(blocks, dtype=jnp.int32)[None, :]
    row_number = (round_number * nr + row_position) * blocks + block_number
    column_updated = jnp.where(row_number[:, :, None] < start_row, so, s)
    round_index = jnp.arange(column_rounds, dtype=jnp.int32)[:, None]
    lane_index = jnp.arange(lanes, dtype=jnp.int32)[None, :]
    column_number = (round_index * nc + column_position) * lanes + lane_index
    row_updated = jnp.where(
        column_number[None] >= start_row + width, jnp.transpose(ro, (1, 0, 2)), flat
    )
    return (
        zo.reshape(vectors_window.shape),
        column_updated.reshape(column_strip.shape),
        row_updated.reshape(row_strip.shape),
    )


def solution(mesh):
    return jax.shard_map(
        body,
        mesh=mesh,
        in_specs=(
            P(None, "row", None, "col"),
            P(None, "row", None, "col"),
            P("row", None, "col", None),
            P("row", "col"),
            P(),
            P(),
        ),
        out_specs=(
            P(None, "row", None, "col"),
            P(None, "row", None, "col"),
            P("row", None, "col", None),
        ),
        check_vma=False,
    )
```

```python
import functools
import jax
import jax.numpy as jnp
from jax import lax
from jax.experimental import pallas as pl
from jax.experimental.pallas import tpu as pltpu
from jax.sharding import PartitionSpec as P

MESH = pl.DeviceIdType.MESH


def drain(ref, sem):
    pltpu.make_async_copy(ref, ref, sem).wait()


def split(x):
    high = x.astype(jnp.bfloat16)
    low = (x - high.astype(jnp.float32)).astype(jnp.bfloat16)
    return high, low


def kernel(
    nr, nc, s_groups, r_first,
    deflated, start, z, s, r, f,
    zo, so, ro,
    fbuf, rot, rh, rl, th, tl,
    zb, sb, rb, zq, sq, rq, rt, rw,
    f_col_send, f_col_recv, f_row_send, f_row_recv, f_pass_send, f_pass_recv,
    in_send, out_send, out_recv, z_recv, s_recv, r_recv,
):
    row = lax.axis_index("row")
    col = lax.axis_index("col")
    z_groups = z.shape[0] // nc
    r_groups = rt.shape[0] // nr
    width = nc * f.shape[1]
    tall = f.shape[0]
    wide = f.shape[1]
    chips = nr // 2
    sibling = row + 1 - 2 * lax.rem(row, 2)

    def col_peer(d):
        return lax.rem(col + d, nc)

    def row_peer(d):
        return lax.rem(row + d, nr)

    def send(src, dst, send_sem, recv_sem, target):
        copy = pltpu.make_async_remote_copy(
            src_ref=src, dst_ref=dst, send_sem=send_sem, recv_sem=recv_sem,
            device_id=target, device_id_type=MESH,
        )
        copy.start()
        return copy

    barrier = pltpu.get_barrier_semaphore()
    for d in range(1, nc):
        pl.semaphore_signal(barrier, inc=1, device_id={"col": col_peer(d)}, device_id_type=MESH)
    for d in range(1, nr):
        pl.semaphore_signal(barrier, inc=1, device_id={"row": row_peer(d)}, device_id_type=MESH)
    pl.semaphore_wait(barrier, nc + nr - 2)

    order = list(range(1, nc))
    half = nc // 2
    base = col // half * half
    mirror = nc - 1 - col
    near = [base + lax.rem(col - base + d, half) for d in range(1, half)]
    send(f, fbuf.at[row, col], f_col_send, f_col_recv.at[0], {"col": mirror})
    for p in near:
        send(f, fbuf.at[row, col], f_col_send, f_col_recv.at[1], {"col": p})

    def z_out(first, last):
        @pl.loop(first, last)
        def _(g):
            for d in order:
                p = col_peer(d)
                send(z.at[g * nc + p], zb.at[g, col], in_send.at[0], z_recv.at[g], {"col": p})

    early = min(2, z_groups)
    z_out(0, early)
    drain(fbuf.at[0, 0], f_col_recv.at[0])
    for p in near:
        send(fbuf.at[row, mirror], fbuf.at[row, mirror], f_col_send, f_col_recv.at[2], {"col": p})
    if early < z_groups:
        z_out(early, z_groups)

    fbuf[row, col] = f[...]
    turn = 8

    def turn_rounds(i):
        return pl.ds(pl.multiple_of(i * turn, turn), turn)

    @pl.loop(r_first * nr // turn, r_groups * nr // turn)
    def _(i):
        rt[turn_rounds(i)] = jnp.swapaxes(r[:, turn_rounds(i), :], 0, 1)

    if r_first:
        @pl.loop(0, r_first * nr // turn)
        def _(i):
            ro[:, turn_rounds(i), :] = r[:, turn_rounds(i), :]

    if s_groups < z_groups:
        @pl.loop(s_groups * nc, z_groups * nc)
        def _(i):
            so[i] = s[i]

    if half > 1:
        drain(fbuf.at[0, pl.ds(0, half - 1)], f_col_recv.at[1])
        drain(fbuf.at[0, pl.ds(0, half - 1)], f_col_recv.at[2])
    send(fbuf.at[row], fbuf.at[row], f_row_send, f_pass_recv.at[0], {"row": sibling})
    for d in range(1, chips):
        send(fbuf.at[row], fbuf.at[row], f_row_send, f_row_recv.at[d], {"row": row_peer(2 * d)})

    if r_first < r_groups:
        @pl.loop(r_first, r_groups)
        def _(g):
            for d in range(1, nr):
                p = row_peer(d)
                send(rt.at[g * nr + p], rb.at[g, row], in_send.at[2], r_recv.at[g], {"row": p})

    if s_groups:
        @pl.loop(0, s_groups)
        def _(g):
            for d in order:
                p = col_peer(d)
                send(s.at[g * nc + p], sb.at[g, col], in_send.at[1], s_recv.at[g], {"col": p})

    for d in range(1, chips):
        drain(fbuf.at[0], f_row_recv.at[d])
        origin = row_peer(nr - 2 * d)
        send(fbuf.at[origin], fbuf.at[origin], f_pass_send, f_pass_recv.at[d], {"row": sibling})
    for d in range(chips):
        drain(fbuf.at[0], f_pass_recv.at[d])

    kept = width - deflated[0]
    squares = jnp.zeros((1, 1), jnp.float32)
    spikes = []
    for c in range(nc):
        lane = lax.broadcasted_iota(jnp.int32, (1, wide), 1) + c * wide
        part = jnp.where(lane < kept, fbuf[0, c, 0:1, :], 0.0)
        squares = squares + jnp.sum(part * part, axis=1, keepdims=True)
        spikes.append((lane, part))
    corner = fbuf[0, 0, 0:1, 0:1]
    magnitude = jnp.sqrt(squares + 1e-06)
    shift = jnp.where(corner >= 0, 1.0, -1.0) * magnitude
    scaling = 2.0 / (squares + 2.0 * jnp.abs(corner) * magnitude + magnitude * magnitude)
    vector = [part + jnp.where(lane == 0, shift, 0.0) for lane, part in spikes]

    @pl.loop(0, nr)
    def _(i):
        image = jnp.zeros((tall, 1), jnp.float32)
        for c in range(nc):
            image = image + jnp.sum(fbuf[i, c] * vector[c], axis=1, keepdims=True)
        image = image * scaling
        rows = pl.ds(pl.multiple_of(i * tall, tall), tall)
        for c in range(nc):
            rot[rows, c * wide:(c + 1) * wide] = fbuf[i, c] - image * vector[c]

    @pl.loop(0, width // 128)
    def _(i):
        rows = pl.ds(pl.multiple_of(i * 128, 128), 128)
        block = rot[rows, :]
        high, low = split(block)
        rh[rows, :] = high
        rl[rows, :] = low
        if r_first < r_groups:
            high, low = split(block.T)
            th[:, rows] = high
            tl[:, rows] = low

    def panel(x, xb, xq, xo, recv, groups, k, limited):
        blk = x.shape[1]

        def back(g):
            for d in order:
                p = col_peer(d)
                send(xq.at[g, p], xo.at[g * nc + col], out_send.at[k], out_recv.at[k], {"col": p})

        @pl.loop(0, groups)
        def _(g):
            xb[g, col] = x[g * nc + col]
            drain(xb.at[g, pl.ds(0, nc - 1)], recv.at[g])
            total = jnp.zeros((blk, width), jnp.float32)
            for c in range(nc):
                high, low = split(xb[g, c])
                rows = slice(c * wide, (c + 1) * wide)
                both = jnp.dot(
                    jnp.concatenate([high, low], axis=0), rh[rows, :],
                    preferred_element_type=jnp.float32,
                )
                total = total + both[:blk] + both[blk:]
                total = total + jnp.dot(high, rl[rows, :], preferred_element_type=jnp.float32)
            if limited:
                first = ((g * nc + col) * nr + row) * blk - start[0]
                moved = lax.broadcasted_iota(jnp.int32, (blk, wide), 0) + first < 0
            for c in range(nc):
                new = total[:, c * wide:(c + 1) * wide]
                xq[g, c] = jnp.where(moved, new, xb[g, c]) if limited else new
            xo[g * nc + col] = xq[g, col]
            @pl.when(g > 0)
            def _():
                back(g - 1)

        back(groups - 1)

    panel(z, zb, zq, zo, z_recv, z_groups, 0, False)

    if r_first < r_groups:
        def r_back(g):
            for d in range(1, nr):
                p = row_peer(d)
                send(rq.at[g, p], rw.at[g * nr + row], out_send.at[2], out_recv.at[2], {"row": p})

        @pl.loop(r_first, r_groups)
        def _(g):
            rb[g, row] = rt[g * nr + row]
            drain(rb.at[g, pl.ds(0, nr - 1)], r_recv.at[g])
            lanes = rt.shape[2]
            high, low = split(rb[g].reshape(width, lanes))
            first = ((g * nr + row) * nc + col) * lanes - start[0] - width
            moved = lax.broadcasted_iota(jnp.int32, (tall, lanes), 1) + first >= 0
            pair = jnp.concatenate([high, low], axis=1)

            @pl.loop(0, nr)
            def _(q):
                rows = pl.ds(pl.multiple_of(q * tall, tall), tall)
                both = jnp.dot(th[rows, :], pair, preferred_element_type=jnp.float32)
                rest = jnp.dot(tl[rows, :], high, preferred_element_type=jnp.float32)
                new = both[:, :lanes] + both[:, lanes:] + rest
                rq[g, q] = jnp.where(moved, new, rb[g, q])

            rw[g * nr + row] = rq[g, row]
            @pl.when(g > r_first)
            def _():
                r_back(g - 1)

        r_back(r_groups - 1)

    if s_groups:
        panel(s, sb, sq, so, s_recv, s_groups, 1, True)

    if r_first < r_groups:
        part = (r_groups - r_first) * (nr - 1)
        drain(rw.at[pl.ds(0, part)], out_recv.at[2])

        @pl.loop(r_first * nr // turn, r_groups * nr // turn)
        def _(i):
            ro[:, turn_rounds(i), :] = jnp.swapaxes(rw[turn_rounds(i)], 0, 1)

        drain(rw.at[pl.ds(0, part)], out_send.at[2])
        drain(rw.at[pl.ds(0, part)], in_send.at[2])
    part = z_groups * (nc - 1)
    drain(zo.at[pl.ds(0, part)], out_recv.at[0])
    drain(zo.at[pl.ds(0, part)], out_send.at[0])
    drain(zo.at[pl.ds(0, part)], in_send.at[0])
    if s_groups:
        part = s_groups * (nc - 1)
        drain(so.at[pl.ds(0, part)], out_recv.at[1])
        drain(so.at[pl.ds(0, part)], out_send.at[1])
        drain(so.at[pl.ds(0, part)], in_send.at[1])
    drain(fbuf.at[0, pl.ds(0, nc - 1)], f_col_send)
    drain(fbuf.at[pl.ds(0, chips)], f_row_send)
    drain(fbuf.at[pl.ds(0, chips - 1)], f_pass_send)


def rotate(nr, nc, s_groups, r_first, ident, z, s, r, f, deflated, start):
    z_groups = z.shape[0] // nc
    tall, column_rounds, lanes = r.shape
    r_groups = column_rounds // nr
    width = nc * f.shape[1]
    vmem = pl.BlockSpec(memory_space=pltpu.VMEM)
    f32 = jnp.float32
    bf16 = jnp.bfloat16
    dma = pltpu.SemaphoreType.DMA
    col_block = (nc,) + z.shape[1:]
    row_block = (nr, tall, lanes)
    return pl.pallas_call(
        functools.partial(kernel, nr, nc, s_groups, r_first),
        out_shape=[jax.ShapeDtypeStruct(x.shape, f32) for x in (z, s, r)],
        in_specs=[pl.BlockSpec(memory_space=pltpu.SMEM)] * 2 + [vmem] * 4,
        out_specs=[vmem] * 3,
        scratch_shapes=[
            pltpu.VMEM((nr, nc) + f.shape, f32),
            pltpu.VMEM((width, width), f32),
            pltpu.VMEM((width, width), bf16),
            pltpu.VMEM((width, width), bf16),
            pltpu.VMEM((width, width), bf16),
            pltpu.VMEM((width, width), bf16),
            pltpu.VMEM((z_groups,) + col_block, f32),
            pltpu.VMEM((z_groups,) + col_block, f32),
            pltpu.VMEM((r_groups,) + row_block, f32),
            pltpu.VMEM((z_groups,) + col_block, f32),
            pltpu.VMEM((z_groups,) + col_block, f32),
            pltpu.VMEM((r_groups,) + row_block, f32),
            pltpu.VMEM((column_rounds, tall, lanes), f32),
            pltpu.VMEM((column_rounds, tall, lanes), f32),
            dma, dma((3,)), dma, dma((nr // 2,)), dma, dma((nr // 2,)),
            dma((3,)), dma((3,)), dma((3,)),
            dma((z_groups,)), dma((z_groups,)), dma((r_groups,)),
        ],
        compiler_params=pltpu.CompilerParams(
            collective_id=ident, has_side_effects=True, vmem_limit_bytes=60 * 1024 * 1024,
        ),
    )(deflated, start, z, s, r, f)


def body(vectors_window, column_strip, row_strip, factor, window_start, deflated):
    nr = lax.axis_size("row")
    nc = lax.axis_size("col")
    start_row = window_start[0]
    rounds, _, blocks, wide = vectors_window.shape
    tall, column_rounds, _, lanes = row_strip.shape
    width = nc * wide
    z = vectors_window.reshape(rounds, blocks, wide)
    s = column_strip.reshape(rounds, blocks, wide)
    r = row_strip.reshape(tall, column_rounds, lanes)
    group_rows = blocks * nr * nc
    group_columns = lanes * nr * nc
    groups = rounds // nc
    branches = [
        functools.partial(
            rotate, nr, nc, k, ((k - 1) * group_rows + 1 + width) // group_columns, k - 1
        )
        for k in range(1, groups + 1)
    ]
    choice = jnp.clip((start_row - 1) // group_rows, 0, groups - 1)
    zo, so, ro = lax.switch(choice, branches, z, s, r, factor, deflated, window_start)
    return (
        zo.reshape(vectors_window.shape),
        so.reshape(column_strip.shape),
        ro.reshape(row_strip.shape),
    )


def solution(mesh):
    return jax.shard_map(
        body,
        mesh=mesh,
        in_specs=(
            P(None, "row", None, "col"),
            P(None, "row", None, "col"),
            P("row", None, "col", None),
            P("row", "col"),
            P(),
            P(),
        ),
        out_specs=(
            P(None, "row", None, "col"),
            P(None, "row", None, "col"),
            P("row", None, "col", None),
        ),
        check_vma=False,
    )
```
